32 devices in a mesh: col: 8 (over y, x, core), grp: 4 (over z).
Axes of the slice: x: 2, y: 2, z: 4, core: 2. Of those that a mesh axis runs over, the one named last changes fastest.
Arguments:
- profiles: float32 [2048, 116], P('col'), may hold values from -6 to 6
- courant: float32 [2048, 58], P('col'), may hold values from -0.7 to 0.7
- owner_map: int32 [2048], replicated, may hold values from 0 to 2047, as said below
- cloud_flags: int32 [2048], P('col'), may hold values 0 or 1
- crm_state: float32 [2, 58, 64, 2048], P(None, None, 'grp', 'col'), may hold values from -6 to 6
Outputs:
- tendency: float32 [2048, 116], P('col')
- crm_final: float32 [2, 58, 64, 2048], P(None, None, 'grp', 'col')
The draws below stay inside these ranges and needn't reach their ends.
Inputs may be any that keep to these rules, and one draw needn't show every extreme that they name: owner_map is a permutation; physics column p lives in span p // 256, element column e in group e // 256; each group hands at most 34 columns to one span, and exactly 34 to some spans, and every span receives exactly 256 columns.
All inputs are finite; a program needn't handle non-finite values. No bound on the sum of `cloud_flags` on one device may be relied on, other than what follows from the above.
Results may differ from the reference program's by a relative error of at most 0.00002.
Values sent between devices are 32-bit elements; how exact they have to be, the bound alone decides.
A program may use at most 64 MiB of HBM per device.

```python
import jax
import jax.numpy as jnp

NX = 64
NZ = 58
COLS_DEV = 256
STEPS = 8
COLUMNS = 2048


def draw_owner_map(key, part):
    per_block = COLS_DEV
    block_count = COLUMNS // COLS_DEV
    mean_load = per_block // block_count
    excess = min(2, mean_load)
    key_pattern, key_offset, key_dest, key_source = jax.random.split(jax.random.fold_in(key, 17), 4)
    block_ids = jnp.arange(block_count, dtype=jnp.int32)
    pattern = jnp.where(block_ids % 2 == 0, mean_load + excess, mean_load - excess).astype(jnp.int32)
    pattern = pattern[jax.random.permutation(key_pattern, block_count)]
    offset_of = jax.random.permutation(key_offset, block_count).astype(jnp.int32)
    counts = pattern[(block_ids[None, :] - offset_of[:, None]) % block_count]
    block_ends = jnp.cumsum(counts, axis=1)
    block_starts = block_ends - counts
    slot_ids = jnp.arange(per_block, dtype=jnp.int32)
    dest_block = jnp.sum((slot_ids[None, :, None] >= block_ends[:, None, :]).astype(jnp.int32), axis=2)
    within = slot_ids[None, :] - jnp.take_along_axis(block_starts, dest_block, axis=1)
    arrival = jnp.cumsum(counts, axis=0) - counts
    slot_in_dest = jnp.take_along_axis(arrival, dest_block, axis=1) + within
    dest_shuffle = jax.vmap(lambda subkey: jax.random.permutation(subkey, per_block))(jax.random.split(key_dest, block_count)).astype(jnp.int32)
    physical = dest_block * per_block + dest_shuffle[dest_block, slot_in_dest]
    source_shuffle = jax.vmap(lambda subkey: jax.random.permutation(subkey, per_block))(jax.random.split(key_source, block_count)).astype(jnp.int32)
    element = block_ids[:, None] * per_block + source_shuffle
    return jnp.zeros((COLUMNS,), jnp.int32).at[element.reshape(-1)].set(physical.reshape(-1).astype(jnp.int32))


def with_ends(values, stream_key, least, largest):
    longest = values.shape.index(max(values.shape))
    spots = []
    for shift in (0, 1):
        where = [jax.random.randint(jax.random.fold_in(stream_key, axis), (), 0, length) for axis, length in enumerate(values.shape)]
        where[longest] = (where[longest] + shift) % values.shape[longest]
        spots.append(tuple(where))
    return values.at[spots[0]].set(least).at[spots[1]].set(largest)


def levels(own_key, extent, pieces, low, high):
    factor_of, own = 1.0, jax.random.fold_in(own_key, 6)
    for axis_at, blocks in pieces:
        draws = jnp.exp(jax.random.uniform(jax.random.fold_in(own, axis_at), (blocks,), jnp.float32, low / len(pieces), high / len(pieces)))
        factor_of = factor_of * jnp.repeat(draws, extent[axis_at] // blocks).reshape([-1 if axis == axis_at else 1 for axis in range(len(extent))])
    return factor_of


def scatter_about(key, extent, width, limit, pieces=(), kind=jnp.bfloat16):
    drawn = width * jax.random.normal(key, extent, jnp.float32)
    if pieces:
        drawn = drawn * levels(key, extent, pieces, -0.22, 0.18)
    return jnp.clip(drawn, -limit, limit).astype(kind)


def setup_inputs(seed: int = 0) -> dict:
    key_of = jax.random.split(jax.random.key(seed), 6)
    return {
        "profiles": scatter_about(key_of[0], (COLUMNS, 2 * NZ), 1.0, 6.0, ((0, 8),), jnp.float32),
        "courant": jnp.clip(jax.random.uniform(key_of[1], (COLUMNS, NZ), jnp.float32, -0.7, 0.7) * levels(key_of[1], (COLUMNS, NZ), ((0, 8),), -0.4, 0.0), -0.7, 0.7),
        "owner_map": draw_owner_map(jax.random.fold_in(key_of[5], 71), 0),
        "cloud_flags": with_ends((jax.random.randint(key_of[3], (COLUMNS,), 0, 2) < 1).astype(jnp.int32), jax.random.fold_in(key_of[3], 1), 0, 1),
        "crm_state": scatter_about(key_of[4], (2, NZ, NX, COLUMNS), 1.0, 6.0, ((2, 4), (3, 8)), jnp.float32),
    }


diffuse_x = 0.25
diffuse_z = 0.2
sat_scale = 0.5
sat_slope = 0.3
cond_rate = 0.5
latent_gain = 0.4


def condense(fields, cloudy):
    energy = fields[0]
    moisture = fields[1]
    saturation = sat_scale * (jnp.exp(sat_slope * energy) - 1.0)
    amount = cond_rate * jnp.maximum(moisture - saturation, 0.0) * cloudy
    return jnp.stack([energy + latent_gain * amount, moisture - amount])


def advance(centre, eastern, western, courant_here, forcing, cloudy):
    upper = jnp.concatenate([centre[:, 1:], centre[:, -1:]], axis=1)
    lower = jnp.concatenate([centre[:, :1], centre[:, :-1]], axis=1)
    stepped = centre + courant_here * ((western - eastern) * 0.5) + diffuse_x * (eastern - 2.0 * centre + western) + diffuse_z * (upper - 2.0 * centre + lower) + forcing
    return condense(stepped, cloudy)


def reference(profiles, courant, owner_map, cloud_flags, crm_state):
    columns = profiles.shape[0]
    phys_prof = jnp.zeros_like(profiles).at[owner_map].set(profiles)
    phys_cour = jnp.zeros_like(courant).at[owner_map].set(courant)
    forcing = (phys_prof.reshape(columns, 2, NZ).transpose(1, 2, 0) / STEPS)[:, :, None, :]
    courant_here = phys_cour.T[None, :, None, :]
    cloudy = cloud_flags.astype(jnp.float32)
    crm_now = crm_state
    for repeat in range(STEPS):
        crm_now = advance(crm_now, jnp.roll(crm_now, -1, axis=2), jnp.roll(crm_now, 1, axis=2), courant_here, forcing, cloudy)
    increment = (jnp.sum(crm_now, axis=2) - jnp.sum(crm_state, axis=2)) / NX
    phys_inc = increment.transpose(2, 0, 1).reshape(columns, 2 * NZ)
    tendency = phys_inc[owner_map]
    return tendency, crm_now
```

```python
import functools

import jax
import jax.numpy as jnp
from jax import lax
from jax.experimental import pallas as pl
from jax.experimental.pallas import tpu as pltpu
from jax.sharding import PartitionSpec as P

STEPS = 8
LANES = 128
MESH = pl.DeviceIdType.MESH
HIGHEST = lax.Precision.HIGHEST

diffuse_x = 0.25
diffuse_z = 0.2
sat_scale = 0.5
sat_slope = 0.3
cond_rate = 0.5
latent_gain = 0.4
LOG2E = 1.4426950408889634


def round_up(n, m):
    return -(-n // m) * m


def cloud_kernel(halo, x_ref, left_ref, right_ref, force_ref, cour_ref, cloud_ref, *rest):
    out_ref, part_ref, buf = rest[-3:]
    levels, cells = x_ref.shape[1:3]
    width = cells + 2 * halo
    half_cloud = cond_rate * cloud_ref[...]

    zeros = jnp.zeros((8, LANES), jnp.float32)

    def fill(z, carry):
        for f in range(2):
            buf[0, f, z, 8 : 8 + halo] = left_ref[f, z]
            buf[0, f, z, 8 + halo : 8 + halo + cells] = x_ref[f, z]
            buf[0, f, z, 8 + halo + cells : 8 + width] = right_ref[f, z]
            for b in range(2):
                buf[b, f, z, 0:8] = zeros
                buf[b, f, z, 8 + width : 16 + width] = zeros
        return carry

    lax.fori_loop(0, levels, fill, 0)

    def stepped(src, z, first, count):
        up = jnp.minimum(z + 1, levels - 1)
        down = jnp.maximum(z - 1, 0)
        c = cour_ref[pl.ds(z, 1), :]
        to_east = diffuse_x + 0.5 * c
        to_west = diffuse_x - 0.5 * c
        new = []
        for f in range(2):
            here = buf[src, f, z, first : first + count]
            west = buf[src, f, z, first - 1 : first + count - 1]
            east = buf[src, f, z, first + 1 : first + count + 1]
            upper = buf[src, f, up, first : first + count]
            lower = buf[src, f, down, first : first + count]
            new.append(
                (1.0 - 2.0 * diffuse_x - 2.0 * diffuse_z) * here
                + (to_east * west + to_west * east)
                + (diffuse_z * (upper + lower) + force_ref[f, pl.ds(z, 1), :])
            )
        energy, moisture = new
        excess = (moisture + sat_scale) - sat_scale * jnp.exp2((sat_slope * LOG2E) * energy)
        amount = jnp.maximum(excess, 0.0) * half_cloud
        return energy + latent_gain * amount, moisture - amount

    def sweep(src, dst):
        def level(z, carry):
            energy, moisture = stepped(src, z, 8, width)
            buf[dst, 0, z, 8 : 8 + width] = energy
            buf[dst, 1, z, 8 : 8 + width] = moisture
            return carry

        lax.fori_loop(0, levels, level, 0, unroll=2)

    sweep(0, 1)

    def pair(i, carry):
        sweep(1, 0)
        sweep(0, 1)
        return carry

    lax.fori_loop(0, (STEPS - 2) // 2, pair, 0)

    def last(z, carry):
        for f, value in enumerate(stepped(1, z, 8 + halo, cells)):
            out_ref[f, z] = value
            part_ref[f, pl.ds(z, 1), :] = jnp.sum(value - x_ref[f, z], axis=0, keepdims=True)
        return carry

    lax.fori_loop(0, levels, last, 0, unroll=2)


def run_cloud(chunk, state, left, right, forcing, courant_here, cloudy, so_far):
    fields, levels, cells, columns = state.shape
    halo = left.shape[2]
    wide = lambda n: pl.BlockSpec((fields, levels, n, LANES), lambda i: (0, 0, 0, chunk))
    one = lambda n: pl.BlockSpec((fields, levels, n, LANES), lambda i: (0, 0, 0, 0))
    in_specs = [
        wide(cells),
        one(halo),
        one(halo),
        pl.BlockSpec((fields, levels, LANES), lambda i: (0, 0, chunk)),
        pl.BlockSpec((levels, LANES), lambda i: (0, chunk)),
        pl.BlockSpec((1, LANES), lambda i: (0, chunk)),
    ]
    args = [state, left, right, forcing, courant_here, cloudy]
    aliases = {}
    if so_far is not None:
        in_specs.append(pl.BlockSpec(memory_space=pl.ANY))
        args.append(so_far)
        aliases = {6: 0}
    work = fields * levels * (cells + 2 * halo) * LANES
    return pl.pallas_call(
        functools.partial(cloud_kernel, halo),
        grid=(1,),
        out_shape=(
            jax.ShapeDtypeStruct(state.shape, jnp.float32),
            jax.ShapeDtypeStruct((fields, levels, LANES), jnp.float32),
        ),
        in_specs=in_specs,
        out_specs=(wide(cells), pl.BlockSpec((fields, levels, LANES), lambda i: (0, 0, 0))),
        scratch_shapes=[pltpu.VMEM((2, fields, levels, cells + 2 * halo + 16, LANES), jnp.float32)],
        input_output_aliases=aliases,
        compiler_params=pltpu.CompilerParams(vmem_limit_bytes=40 * 2**20),
        cost_estimate=pl.CostEstimate(
            flops=28 * STEPS * work // 2, bytes_accessed=8 * work, transcendentals=STEPS * work // 2
        ),
    )(*args)


def tail_kernel(cells_all, part_ref, t_ref, r_ref, out_ref, mine, inc, heap, pack, land, sems):
    rows, lanes = part_ref.shape
    groups, cap = land.shape[:2]
    grp_count = lax.axis_size("grp")
    share = rows // grp_count
    z = lax.axis_index("grp")
    c = lax.axis_index("col")
    barrier = pltpu.get_barrier_semaphore()
    for k in range(1, grp_count):
        pl.semaphore_signal(
            barrier, inc=1, device_id={"grp": lax.rem(z + k, grp_count)}, device_id_type=MESH
        )
    for k in range(1, groups):
        pl.semaphore_signal(
            barrier, inc=1, device_id={"col": lax.rem(c + k, groups)}, device_id_type=MESH
        )
    pl.semaphore_wait(barrier, grp_count - 1 + groups - 1)

    def block(i):
        return pl.ds(pl.multiple_of(i * share, share), share)

    scatter = []
    for k in range(1, grp_count):
        peer = lax.rem(z + k, grp_count)
        copy = pltpu.make_async_remote_copy(
            src_ref=part_ref.at[block(peer)],
            dst_ref=heap.at[k - 1],
            send_sem=sems.at[0, k],
            recv_sem=sems.at[1, k],
            device_id={"grp": peer},
            device_id_type=MESH,
        )
        copy.start()
        scatter.append(copy)
    total = part_ref[block(z), :]
    for k, copy in enumerate(scatter):
        copy.wait_recv()
        total = total + heap[k]
    mine[...] = total / cells_all
    inc[block(z), :] = total / cells_all
    spread = []
    for k in range(1, grp_count):
        copy = pltpu.make_async_remote_copy(
            src_ref=mine,
            dst_ref=inc.at[block(z)],
            send_sem=sems.at[2, k],
            recv_sem=sems.at[3, k],
            device_id={"grp": lax.rem(z + k, grp_count)},
            device_id_type=MESH,
        )
        copy.start()
        spread.append(copy)
    for copy in spread:
        copy.wait_recv()
    pack[...] = jnp.dot(
        t_ref[...], inc[...], precision=HIGHEST, preferred_element_type=jnp.float32
    ).reshape(groups, cap, lanes)
    returns = []
    for k in range(1, groups):
        peer = lax.rem(c + k, groups)
        copy = pltpu.make_async_remote_copy(
            src_ref=pack.at[peer],
            dst_ref=land.at[c],
            send_sem=sems.at[4, k],
            recv_sem=sems.at[5, k],
            device_id={"col": peer},
            device_id_type=MESH,
        )
        copy.start()
        returns.append(copy)
    land[c] = pack[c]
    for copy in returns:
        copy.wait_recv()
    out = lax.dot_general(
        r_ref[...],
        land[...].reshape(groups * cap, lanes),
        (((0,), (0,)), ((), ())),
        precision=HIGHEST,
        preferred_element_type=jnp.float32,
    )
    out_ref[...] = out[:, : out_ref.shape[1]]
    for copy in scatter + spread + returns:
        copy.wait_send()


def run_tail(cells_all, partial, take, give, width):
    rows, lanes = partial.shape
    groups = lax.axis_size("col")
    grp_count = lax.axis_size("grp")
    cap = take.shape[0] // groups
    vmem = pl.BlockSpec(memory_space=pltpu.VMEM)
    return pl.pallas_call(
        functools.partial(tail_kernel, cells_all),
        out_shape=jax.ShapeDtypeStruct((rows, width), jnp.float32),
        in_specs=[vmem] * 3,
        out_specs=vmem,
        scratch_shapes=[
            pltpu.VMEM((rows // grp_count, lanes), jnp.float32),
            pltpu.VMEM((rows, lanes), jnp.float32),
            pltpu.VMEM((grp_count - 1, rows // grp_count, lanes), jnp.float32),
            pltpu.VMEM((groups, cap, lanes), jnp.float32),
            pltpu.VMEM((groups, cap, lanes), jnp.float32),
            pltpu.SemaphoreType.DMA((6, max(grp_count, groups))),
        ],
        compiler_params=pltpu.CompilerParams(collective_id=0, has_side_effects=True),
    )(partial, take, give)


def ring_halo(part, depth):
    peers, cells = lax.axis_size("grp"), part.shape[2]
    lefts, rights = [], []
    need, hop = depth, 1
    while need > 0:
        n = min(need, cells)
        up = [(i, (i + hop) % peers) for i in range(peers)]
        down = [(j, i) for i, j in up]
        lefts.insert(0, lax.ppermute(part[:, :, cells - n :], "grp", up))
        rights.append(lax.ppermute(part[:, :, :n], "grp", down))
        need, hop = need - n, hop + 1
    join = lambda xs: xs[0] if len(xs) == 1 else jnp.concatenate(xs, axis=2)
    return join(lefts), join(rights)


def on_device(profiles, courant, owner_map, cloud_flags, crm_state):
    columns = profiles.shape[0]
    levels = courant.shape[1]
    groups = lax.axis_size("col")
    me = lax.axis_index("col")
    per_peer = columns // groups
    cap = round_up(per_peer + min(2, per_peer), 8)
    chunks = columns // LANES

    halos = []
    for i in range(chunks):
        halos.append(ring_halo(crm_state[..., i * LANES : (i + 1) * LANES], STEPS))

    ids = jnp.arange(groups, dtype=jnp.int32)
    slots = jnp.arange(cap, dtype=jnp.int32)
    spots = jnp.arange(columns, dtype=jnp.int32)
    earlier = (spots[:, None] < spots[None, :]).astype(jnp.float32)
    mine = lax.dynamic_slice_in_dim(owner_map, me * columns, columns)
    blocks = owner_map.reshape(groups, columns)

    def places(hits):
        rank = jnp.dot(hits.astype(jnp.float32), earlier).astype(jnp.int32)
        return hits[:, None, :] & (rank[:, None, :] == slots[None, :, None])

    give = places((mine // columns)[None, :] == ids[:, None])
    give = give.reshape(groups * cap, columns).astype(jnp.float32)
    landing = places(blocks // columns == me)
    spot = jnp.sum(jnp.where(landing, (blocks - me * columns + 1)[:, None, :], 0), axis=2)
    take = (spot.reshape(groups * cap)[:, None] == spots[None, :] + 1).astype(jnp.float32)

    both = jnp.concatenate([profiles, courant], axis=1)
    out = jnp.dot(give, both, precision=HIGHEST).reshape(groups, cap, 3 * levels)
    got = lax.all_to_all(out, "col", split_axis=0, concat_axis=0, tiled=True)
    phys = lax.dot_general(
        got.reshape(groups * cap, 3 * levels), take, (((0,), (0,)), ((), ())), precision=HIGHEST
    )
    forcing = phys[: 2 * levels].reshape(2, levels, columns) / STEPS
    courant_here = phys[2 * levels :]
    cloudy = cloud_flags.astype(jnp.float32)[None, :]

    final, parts = None, []
    for i, (left, right) in enumerate(halos):
        final, part = run_cloud(
            i, crm_state, left, right, forcing, courant_here, cloudy, final
        )
        parts.append(part.reshape(2 * levels, LANES).T)
    partial = jnp.concatenate(parts, axis=0)
    partial = jnp.pad(partial, ((0, 0), (0, round_up(2 * levels, LANES) - 2 * levels)))
    cells_all = crm_state.shape[2] * lax.axis_size("grp")
    tendency = run_tail(float(cells_all), partial, take, give, 2 * levels)
    return tendency, final


def solution(mesh):
    placed = (P("col", None), P("col", None), P(), P("col"), P(None, None, "grp", "col"))
    return jax.shard_map(
        on_device,
        mesh=mesh,
        in_specs=placed,
        out_specs=(P("col", None), P(None, None, "grp", "col")),
        check_vma=False,
    )
```

```python
import functools

import jax
import jax.numpy as jnp
from jax import lax
from jax.experimental import pallas as pl
from jax.experimental.pallas import tpu as pltpu
from jax.sharding import PartitionSpec as P

STEPS = 8
DEPTH = 4
LANES = 128
TOP = 8
MESH = pl.DeviceIdType.MESH
HIGHEST = lax.Precision.HIGHEST

diffuse_x = 0.25
diffuse_z = 0.2
sat_scale = 0.5
sat_slope = 0.3
cond_rate = 0.5
latent_gain = 0.4
LOG2E = 1.4426950408889634


def round_up(n, m):
    return -(-n // m) * m


def contract(a, b, dims):
    return lax.dot_general(
        a, b, (dims, ((), ())), precision=HIGHEST, preferred_element_type=jnp.float32
    )


def window_kernel(
    depth,
    prof_ref,
    cour_ref,
    owner_ref,
    cloud_ref,
    x_ref,
    tend_ref,
    final_ref,
    xs,
    outs,
    buf,
    sends,
    gets,
    give,
    take,
    fsend,
    fland,
    force,
    wind,
    part,
    heap,
    mine,
    inc,
    pack,
    land,
    local_sem,
    halo_sem,
    force_sem,
    sum_sem,
    back_sem,
):
    fields, levels, cells = xs.shape[1:4]
    chunks = xs.shape[0]
    groups, cap = fland.shape[:2]
    columns = owner_ref.shape[1]
    peers = lax.axis_size("grp")
    z_me = lax.axis_index("grp")
    c_me = lax.axis_index("col")
    rounds = STEPS // depth
    width = cells + 2 * depth
    span = lambda i: pl.ds(i * LANES, LANES)

    loads = []
    for c in range(chunks):
        load = pltpu.make_async_copy(
            x_ref.at[:, :, :, span(c)], xs.at[c], local_sem.at[0, c]
        )
        load.start()
        loads.append(load)

    barrier = pltpu.get_barrier_semaphore()
    for k in range(1, peers):
        pl.semaphore_signal(
            barrier, inc=1, device_id={"grp": lax.rem(z_me + k, peers)}, device_id_type=MESH
        )
    for k in range(1, groups):
        pl.semaphore_signal(
            barrier, inc=1, device_id={"col": lax.rem(c_me + k, groups)}, device_id_type=MESH
        )

    def halo_copies(c, r):
        copies = []
        for side in range(2):
            peer = lax.rem(z_me + (peers - 1 if side == 0 else 1), peers)
            copies.append(
                pltpu.make_async_remote_copy(
                    src_ref=sends.at[c, r, side],
                    dst_ref=gets.at[c, r, side],
                    send_sem=halo_sem.at[0, c, r, side],
                    recv_sem=halo_sem.at[1, c, r, side],
                    device_id={"grp": peer},
                    device_id_type=MESH,
                )
            )
        return copies

    waits = []
    for c in range(chunks):
        loads[c].wait()

        def fill(z, carry):
            for f in range(fields):
                x = xs[c, f, z]
                buf[c, 0, f, z, TOP : TOP + cells] = x
                sends[c, 0, 0, f, z] = x[:depth]
                sends[c, 0, 1, f, z] = x[cells - depth :]
            return carry

        lax.fori_loop(0, levels, fill, 0)
        if c == 0:
            pl.semaphore_wait(barrier, peers - 1 + groups - 1)
        for copy in halo_copies(c, 0):
            copy.start()
            waits.append(copy)

    owner = owner_ref[...]
    own_row = owner_ref[pl.ds(c_me, 1), :]
    group_ids = lax.broadcasted_iota(jnp.int32, (groups, columns), 0)
    earlier = (
        lax.broadcasted_iota(jnp.int32, (columns, columns), 0)
        < lax.broadcasted_iota(jnp.int32, (columns, columns), 1)
    ).astype(jnp.float32)
    slot = lax.broadcasted_iota(jnp.int32, (cap, columns), 0).astype(jnp.float32)
    spot = lax.broadcasted_iota(jnp.int32, (cap, columns), 1).astype(jnp.float32) + 1.0

    def ranked(hits):
        rank = jnp.dot(hits, earlier, preferred_element_type=jnp.float32)
        return jnp.where(hits > 0.5, rank, -1.0)

    low = own_row - group_ids * columns
    order = ranked(jnp.where((low >= 0) & (low < columns), 1.0, 0.0))
    for q in range(groups):
        give[q * cap : (q + 1) * cap, :] = jnp.where(order[q : q + 1] == slot, 1.0, 0.0)

    for f, ref in ((0, prof_ref), (1, cour_ref)):
        lines = ref.shape[0]
        fsend[:, :, f * LANES : f * LANES + lines] = contract(
            give[...], ref[...], ((1,), (1,))
        ).reshape(groups, cap, lines)
    shares = []
    for k in range(1, groups):
        peer = lax.rem(c_me + k, groups)
        copy = pltpu.make_async_remote_copy(
            src_ref=fsend.at[peer],
            dst_ref=fland.at[c_me],
            send_sem=force_sem.at[0, k],
            recv_sem=force_sem.at[1, k],
            device_id={"col": peer},
            device_id_type=MESH,
        )
        copy.start()
        shares.append(copy)
    waits += shares
    fland[c_me] = fsend[c_me]

    local = owner - c_me * columns
    order = ranked(jnp.where((local >= 0) & (local < columns), 1.0, 0.0))
    place = (local + 1).astype(jnp.float32)
    for q in range(groups):
        chosen = jnp.where(order[q : q + 1] == slot, place[q : q + 1], 0.0)
        chosen = jnp.sum(chosen, axis=1, keepdims=True)
        take[q * cap : (q + 1) * cap, :] = jnp.where(chosen == spot, 1.0, 0.0)

    for copy in shares:
        copy.wait_recv()
    phys = contract(
        fland[:, :, :LANES].reshape(groups * cap, LANES), take[...], ((0,), (0,))
    )
    for f in range(fields):
        for c in range(chunks):
            force[c, f] = (
                phys[f * levels : (f + 1) * levels, c * LANES : (c + 1) * LANES] / STEPS
            )
    phys = contract(
        fland[:, :, LANES:].reshape(groups * cap, LANES), take[...], ((0,), (0,))
    )
    for c in range(chunks):
        wind[c] = phys[:levels, c * LANES : (c + 1) * LANES]
    half_cloud = cond_rate * cloud_ref[...].astype(jnp.float32)

    def stepped(c, src, z, count):
        up = jnp.minimum(z + 1, levels - 1)
        down = jnp.maximum(z - 1, 0)
        lanes = slice(c * LANES, (c + 1) * LANES)
        speed = 0.5 * wind[c, pl.ds(z, 1), :]
        new = []
        for f in range(fields):
            here = buf[c, src, f, z, TOP : TOP + count]
            west = buf[c, src, f, z, TOP - 1 : TOP - 1 + count]
            east = buf[c, src, f, z, TOP + 1 : TOP + 1 + count]
            upper = buf[c, src, f, up, TOP : TOP + count]
            lower = buf[c, src, f, down, TOP : TOP + count]
            new.append(
                (1.0 - 2.0 * diffuse_x - 2.0 * diffuse_z) * here
                + ((diffuse_x + speed) * west + (diffuse_x - speed) * east)
                + (diffuse_z * (upper + lower) + force[c, f, pl.ds(z, 1), :])
            )
        energy, moisture = new
        excess = (moisture + sat_scale) - sat_scale * jnp.exp2((sat_slope * LOG2E) * energy)
        amount = jnp.maximum(excess, 0.0) * half_cloud[:, lanes]
        return energy + latent_gain * amount, moisture - amount

    def sweep(c, src):
        def level(z, carry):
            for f, value in enumerate(stepped(c, src, z, width)):
                buf[c, 1 - src, f, z, TOP : TOP + width] = value
                buf[c, 1 - src, f, z, TOP - 1 : TOP] = value[width - 1 :]
                buf[c, 1 - src, f, z, TOP + width : TOP + width + 1] = value[:1]
            return carry

        lax.fori_loop(0, levels, level, 0, unroll=2)

    def last(c, src):
        def level(z, carry):
            for f, value in enumerate(stepped(c, src, z, cells)):
                outs[c, f, z] = value
                part[c, pl.ds(f * levels + z, 1), :] = jnp.sum(
                    value - xs[c, f, z], axis=0, keepdims=True
                )
            return carry

        lax.fori_loop(0, levels, level, 0, unroll=2)

    lines = part.shape[1] // peers
    block = lambda i: pl.ds(pl.multiple_of(i * lines, lines), lines)

    def sum_copies(c, phase):
        copies = []
        for k in range(1, peers):
            peer = lax.rem(z_me + k, peers)
            if phase == 0:
                source, target = part.at[c, block(peer)], heap.at[c, k]
            else:
                source, target = mine.at[c], inc.at[c, block(z_me)]
            copies.append(
                pltpu.make_async_remote_copy(
                    src_ref=source,
                    dst_ref=target,
                    send_sem=sum_sem.at[phase, 0, c, k],
                    recv_sem=sum_sem.at[phase, 1, c, k],
                    device_id={"grp": peer},
                    device_id_type=MESH,
                )
            )
        for copy in copies:
            copy.start()
            waits.append(copy)
        return copies

    def add_up(c, scatter):
        total = part[c, block(z_me), :]
        for k, copy in enumerate(scatter):
            copy.wait_recv()
            total = total + heap[c, k + 1]
        total = total / (cells * peers)
        mine[c] = total
        inc[c, block(z_me), :] = total
        return sum_copies(c, 1)

    pad_rows = part.shape[1] - fields * levels
    if pad_rows:
        for c in range(chunks):
            part[c, fields * levels :, :] = jnp.zeros((pad_rows, LANES), jnp.float32)

    scatters, gathers, stores = [], [], []
    for r in range(rounds):
        for c in range(chunks):
            for copy in halo_copies(c, r):
                copy.wait_recv()
            src = (r * depth) % 2

            def widen(z, carry):
                for f in range(fields):
                    right = gets[c, r, 0, f, z]
                    left = gets[c, r, 1, f, z]
                    buf[c, src, f, z, TOP + cells : TOP + cells + depth] = right
                    buf[c, src, f, z, TOP + cells + depth : TOP + width] = left
                    buf[c, src, f, z, TOP - 1 : TOP] = left[depth - 1 :]
                    buf[c, src, f, z, TOP + width : TOP + width + 1] = buf[
                        c, src, f, z, TOP : TOP + 1
                    ]
                return carry

            lax.fori_loop(0, levels, widen, 0)
            final_round = r == rounds - 1
            if final_round and c > 0:
                gathers += add_up(c - 1, scatters[c - 1])
            for s in range(depth - 1 if final_round else depth):
                sweep(c, (src + s) % 2)
            src = (src + depth - (1 if final_round else 0)) % 2
            if not final_round:

                def narrow(z, carry):
                    for f in range(fields):
                        sends[c, r + 1, 0, f, z] = buf[c, src, f, z, TOP : TOP + depth]
                        sends[c, r + 1, 1, f, z] = buf[
                            c, src, f, z, TOP + cells - depth : TOP + cells
                        ]
                    return carry

                lax.fori_loop(0, levels, narrow, 0)
                for copy in halo_copies(c, r + 1):
                    copy.start()
                    waits.append(copy)
            else:
                last(c, src)
                scatters.append(sum_copies(c, 0))
                store = pltpu.make_async_copy(
                    outs.at[c], final_ref.at[:, :, :, span(c)], local_sem.at[1, c]
                )
                store.start()
                stores.append(store)
    gathers += add_up(chunks - 1, scatters[chunks - 1])
    for copy in gathers:
        copy.wait_recv()
    packed = 0.0
    for c in range(chunks):
        packed = packed + contract(
            take[:, c * LANES : (c + 1) * LANES], inc[c], ((1,), (1,))
        )
    pack[...] = packed.reshape(pack.shape)
    returns = []
    for k in range(1, groups):
        peer = lax.rem(c_me + k, groups)
        copy = pltpu.make_async_remote_copy(
            src_ref=pack.at[peer],
            dst_ref=land.at[c_me],
            send_sem=back_sem.at[0, k],
            recv_sem=back_sem.at[1, k],
            device_id={"col": peer},
            device_id_type=MESH,
        )
        copy.start()
        returns.append(copy)
    waits += returns
    land[c_me] = pack[c_me]
    for copy in returns:
        copy.wait_recv()
    back = contract(land[...].reshape(groups * cap, land.shape[2]), give[...], ((0,), (0,)))
    tend_ref[...] = back[: fields * levels]
    for copy in waits:
        copy.wait_send()
    for store in stores:
        store.wait()


def on_device(profiles, courant, owner_map, cloud_flags, crm_state):
    columns = profiles.shape[0]
    fields, levels, cells = crm_state.shape[:3]
    groups = lax.axis_size("col")
    peers = lax.axis_size("grp")
    per_peer = columns // groups
    cap = round_up(per_peer + min(2, per_peer), 8)
    chunks = columns // LANES
    depth = min(DEPTH, cells)
    rounds = STEPS // depth
    rows = round_up(fields * levels, 8 * peers)
    wide = round_up(rows, LANES)
    f32 = lambda *shape: pltpu.VMEM(shape, jnp.float32)
    dma = lambda *shape: pltpu.SemaphoreType.DMA(shape)
    vmem = pl.BlockSpec(memory_space=pltpu.VMEM)
    anywhere = pl.BlockSpec(memory_space=pl.ANY)
    tall = round_up(TOP + cells + 2 * depth + 1, 8)
    tendency, final = pl.pallas_call(
        functools.partial(window_kernel, depth),
        out_shape=(
            jax.ShapeDtypeStruct((fields * levels, columns), jnp.float32),
            jax.ShapeDtypeStruct(crm_state.shape, jnp.float32),
        ),
        in_specs=[vmem, vmem, vmem, vmem, anywhere],
        out_specs=(vmem, anywhere),
        scratch_shapes=[
            f32(chunks, fields, levels, cells, LANES),
            f32(chunks, fields, levels, cells, LANES),
            f32(chunks, 2, fields, levels, tall, LANES),
            f32(chunks, rounds, 2, fields, levels, depth, LANES),
            f32(chunks, rounds, 2, fields, levels, depth, LANES),
            f32(groups * cap, columns),
            f32(groups * cap, columns),
            f32(groups, cap, 2 * LANES),
            f32(groups, cap, 2 * LANES),
            f32(chunks, fields, levels, LANES),
            f32(chunks, levels, LANES),
            f32(chunks, rows, LANES),
            f32(chunks, peers, rows // peers, LANES),
            f32(chunks, rows // peers, LANES),
            f32(chunks, rows, LANES),
            f32(groups, cap, rows),
            f32(groups, cap, rows),
            dma(2, chunks),
            dma(2, chunks, rounds, 2),
            dma(2, groups),
            dma(2, 2, chunks, peers),
            dma(2, groups),
        ],
        compiler_params=pltpu.CompilerParams(
            collective_id=0, has_side_effects=True, vmem_limit_bytes=56 * 2**20
        ),
    )(profiles.T, courant.T, owner_map.reshape(groups, columns), cloud_flags[None, :], crm_state)
    return tendency.T, final


def solution(mesh):
    placed = (P("col", None), P("col", None), P(), P("col"), P(None, None, "grp", "col"))
    return jax.shard_map(
        on_device,
        mesh=mesh,
        in_specs=placed,
        out_specs=(P("col", None), P(None, None, "grp", "col")),
        check_vma=False,
    )
```

```python
import functools

import jax
import jax.numpy as jnp
from jax import lax
from jax.experimental import pallas as pl
from jax.experimental.pallas import tpu as pltpu
from jax.sharding import PartitionSpec as P

STEPS = 8
DEPTH = 4
LANES = 128
LIMIT = 36 * 2**20
TOP = 8
MESH = pl.DeviceIdType.MESH
HIGHEST = lax.Precision.HIGHEST

diffuse_x = 0.25
diffuse_z = 0.2
sat_scale = 0.5
sat_slope = 0.3
cond_rate = 0.5
latent_gain = 0.4
LOG2E = 1.4426950408889634


def round_up(n, m):
    return -(-n // m) * m


def contract(a, b, dims):
    return lax.dot_general(
        a, b, (dims, ((), ())), precision=HIGHEST, preferred_element_type=jnp.float32
    )


def window_kernel(
    depth,
    prof_ref,
    cour_ref,
    owner_ref,
    cloud_ref,
    x_ref,
    land,
    give,
    final_ref,
    xs,
    outs,
    buf,
    sends,
    gets,
    take,
    fsend,
    fland,
    force,
    wind,
    part,
    heap,
    mine,
    inc,
    pack,
    local_sem,
    halo_sem,
    force_sem,
    sum_sem,
    back_sem,
):
    fields, levels, cells = xs.shape[1:4]
    chunks = xs.shape[0]
    groups, cap = fland.shape[:2]
    columns = chunks * LANES
    peers = lax.axis_size("grp")
    z_me = lax.axis_index("grp")
    c_me = lax.axis_index("col")
    rounds = STEPS // depth
    width = cells + 2 * depth
    span = lambda i: pl.ds(i * LANES, LANES)

    loads = []
    for c in range(chunks):
        load = pltpu.make_async_copy(
            x_ref.at[:, :, :, span(c)], xs.at[c], local_sem.at[0, c]
        )
        load.start()
        loads.append(load)

    barrier = pltpu.get_barrier_semaphore()
    for k in range(1, peers):
        pl.semaphore_signal(
            barrier, inc=1, device_id={"grp": lax.rem(z_me + k, peers)}, device_id_type=MESH
        )
    for k in range(1, groups):
        pl.semaphore_signal(
            barrier, inc=1, device_id={"col": lax.rem(c_me + k, groups)}, device_id_type=MESH
        )

    def halo_copies(c, r):
        copies = []
        for side in range(2):
            peer = lax.rem(z_me + (peers - 1 if side == 0 else 1), peers)
            copies.append(
                pltpu.make_async_remote_copy(
                    src_ref=sends.at[c, r, side],
                    dst_ref=gets.at[c, r, side],
                    send_sem=halo_sem.at[0, c, r, side],
                    recv_sem=halo_sem.at[1, c, r, side],
                    device_id={"grp": peer},
                    device_id_type=MESH,
                )
            )
        return copies

    waits = []
    for c in range(chunks):
        loads[c].wait()

        def fill(z, carry):
            for f in range(fields):
                x = xs[c, f, z]
                buf[c, 0, f, z, TOP : TOP + cells] = x
                sends[c, 0, 0, f, z] = x[:depth]
                sends[c, 0, 1, f, z] = x[cells - depth :]
            return carry

        lax.fori_loop(0, levels, fill, 0)
        if c == 0:
            pl.semaphore_wait(barrier, peers - 1 + groups - 1)
        for copy in halo_copies(c, 0):
            copy.start()
            waits.append(copy)

    owner = jnp.concatenate(
        [owner_ref[pl.ds(c, groups, stride=chunks), :] for c in range(chunks)], axis=1
    )
    own_row = jnp.concatenate(
        [owner_ref[pl.ds(c_me * chunks + c, 1), :] for c in range(chunks)], axis=1
    )
    group_ids = lax.broadcasted_iota(jnp.int32, (groups, columns), 0)
    earlier = (
        lax.broadcasted_iota(jnp.int32, (columns, columns), 0)
        < lax.broadcasted_iota(jnp.int32, (columns, columns), 1)
    ).astype(jnp.float32)
    slot = lax.broadcasted_iota(jnp.int32, (cap, columns), 0).astype(jnp.float32)
    spot = lax.broadcasted_iota(jnp.int32, (cap, columns), 1).astype(jnp.float32) + 1.0

    def ranked(hits):
        rank = jnp.dot(hits, earlier, preferred_element_type=jnp.float32)
        return jnp.where(hits > 0.5, rank, -1.0)

    low = own_row - group_ids * columns
    order = ranked(jnp.where((low >= 0) & (low < columns), 1.0, 0.0))
    for q in range(groups):
        give[q * cap : (q + 1) * cap, :] = jnp.where(order[q : q + 1] == slot, 1.0, 0.0)

    for f, ref in ((0, prof_ref), (1, cour_ref)):
        lines = ref.shape[0]
        fsend[:, :, f * LANES : f * LANES + lines] = contract(
            give[...], ref[...], ((1,), (1,))
        ).reshape(groups, cap, lines)
    shares = []
    for k in range(1, groups):
        peer = lax.rem(c_me + k, groups)
        copy = pltpu.make_async_remote_copy(
            src_ref=fsend.at[peer],
            dst_ref=fland.at[c_me],
            send_sem=force_sem.at[0, k],
            recv_sem=force_sem.at[1, k],
            device_id={"col": peer},
            device_id_type=MESH,
        )
        copy.start()
        shares.append(copy)
    waits += shares
    fland[c_me] = fsend[c_me]

    local = owner - c_me * columns
    order = ranked(jnp.where((local >= 0) & (local < columns), 1.0, 0.0))
    place = (local + 1).astype(jnp.float32)
    for q in range(groups):
        chosen = jnp.where(order[q : q + 1] == slot, place[q : q + 1], 0.0)
        chosen = jnp.sum(chosen, axis=1, keepdims=True)
        take[q * cap : (q + 1) * cap, :] = jnp.where(chosen == spot, 1.0, 0.0)

    for copy in shares:
        copy.wait_recv()
    phys = contract(
        fland[:, :, :LANES].reshape(groups * cap, LANES), take[...], ((0,), (0,))
    )
    for f in range(fields):
        for c in range(chunks):
            force[c, f] = (
                phys[f * levels : (f + 1) * levels, c * LANES : (c + 1) * LANES] / STEPS
            )
    phys = contract(
        fland[:, :, LANES:].reshape(groups * cap, LANES), take[...], ((0,), (0,))
    )
    for c in range(chunks):
        wind[c] = phys[:levels, c * LANES : (c + 1) * LANES]
    half_cloud = cond_rate * cloud_ref[...].astype(jnp.float32)

    def stepped(c, src, z, count):
        up = jnp.minimum(z + 1, levels - 1)
        down = jnp.maximum(z - 1, 0)
        lanes = slice(c * LANES, (c + 1) * LANES)
        speed = 0.5 * wind[c, pl.ds(z, 1), :]
        new = []
        for f in range(fields):
            here = buf[c, src, f, z, TOP : TOP + count]
            west = buf[c, src, f, z, TOP - 1 : TOP - 1 + count]
            east = buf[c, src, f, z, TOP + 1 : TOP + 1 + count]
            upper = buf[c, src, f, up, TOP : TOP + count]
            lower = buf[c, src, f, down, TOP : TOP + count]
            new.append(
                (1.0 - 2.0 * diffuse_x - 2.0 * diffuse_z) * here
                + ((diffuse_x + speed) * west + (diffuse_x - speed) * east)
                + (diffuse_z * (upper + lower) + force[c, f, pl.ds(z, 1), :])
            )
        energy, moisture = new
        excess = (moisture + sat_scale) - sat_scale * jnp.exp2((sat_slope * LOG2E) * energy)
        amount = jnp.maximum(excess, 0.0) * half_cloud[:, lanes]
        return energy + latent_gain * amount, moisture - amount

    def sweep(c, src):
        def level(z, carry):
            for f, value in enumerate(stepped(c, src, z, width)):
                buf[c, 1 - src, f, z, TOP : TOP + width] = value
                buf[c, 1 - src, f, z, TOP - 1 : TOP] = value[width - 1 :]
                buf[c, 1 - src, f, z, TOP + width : TOP + width + 1] = value[:1]
            return carry

        lax.fori_loop(0, levels, level, 0, unroll=2)

    def last(c, src):
        def level(z, carry):
            for f, value in enumerate(stepped(c, src, z, cells)):
                outs[c, f, z] = value
                part[c, pl.ds(f * levels + z, 1), :] = jnp.sum(
                    value - xs[c, f, z], axis=0, keepdims=True
                )
            return carry

        lax.fori_loop(0, levels, level, 0, unroll=2)

    lines = part.shape[1] // peers
    block = lambda i: pl.ds(pl.multiple_of(i * lines, lines), lines)

    def sum_copies(c, phase):
        copies = []
        for k in range(1, peers):
            peer = lax.rem(z_me + k, peers)
            if phase == 0:
                source, target = part.at[c, block(peer)], heap.at[c, k]
            else:
                source, target = mine.at[c], inc.at[c, block(z_me)]
            copies.append(
                pltpu.make_async_remote_copy(
                    src_ref=source,
                    dst_ref=target,
                    send_sem=sum_sem.at[phase, 0, c, k],
                    recv_sem=sum_sem.at[phase, 1, c, k],
                    device_id={"grp": peer},
                    device_id_type=MESH,
                )
            )
        for copy in copies:
            copy.start()
            waits.append(copy)
        return copies

    def add_up(c, scatter):
        total = part[c, block(z_me), :]
        for k, copy in enumerate(scatter):
            copy.wait_recv()
            total = total + heap[c, k + 1]
        total = total / (cells * peers)
        mine[c] = total
        inc[c, block(z_me), :] = total
        return sum_copies(c, 1)

    pad_rows = part.shape[1] - fields * levels
    if pad_rows:
        for c in range(chunks):
            part[c, fields * levels :, :] = jnp.zeros((pad_rows, LANES), jnp.float32)

    scatters, gathers, stores = [], [], []
    for r in range(rounds):
        for c in range(chunks):
            for copy in halo_copies(c, r):
                copy.wait_recv()
            src = (r * depth) % 2

            def widen(z, carry):
                for f in range(fields):
                    right = gets[c, r, 0, f, z]
                    left = gets[c, r, 1, f, z]
                    buf[c, src, f, z, TOP + cells : TOP + cells + depth] = right
                    buf[c, src, f, z, TOP + cells + depth : TOP + width] = left
                    buf[c, src, f, z, TOP - 1 : TOP] = left[depth - 1 :]
                    buf[c, src, f, z, TOP + width : TOP + width + 1] = buf[
                        c, src, f, z, TOP : TOP + 1
                    ]
                return carry

            lax.fori_loop(0, levels, widen, 0)
            final_round = r == rounds - 1
            if final_round and c > 0:
                gathers += add_up(c - 1, scatters[c - 1])
            for s in range(depth - 1 if final_round else depth):
                sweep(c, (src + s) % 2)
            src = (src + depth - (1 if final_round else 0)) % 2
            if not final_round:

                def narrow(z, carry):
                    for f in range(fields):
                        sends[c, r + 1, 0, f, z] = buf[c, src, f, z, TOP : TOP + depth]
                        sends[c, r + 1, 1, f, z] = buf[
                            c, src, f, z, TOP + cells - depth : TOP + cells
                        ]
                    return carry

                lax.fori_loop(0, levels, narrow, 0)
                for copy in halo_copies(c, r + 1):
                    copy.start()
                    waits.append(copy)
            else:
                last(c, src)
                scatters.append(sum_copies(c, 0))
                store = pltpu.make_async_copy(
                    outs.at[c], final_ref.at[:, :, :, span(c)], local_sem.at[1, c]
                )
                store.start()
                stores.append(store)
    gathers += add_up(chunks - 1, scatters[chunks - 1])
    for copy in gathers:
        copy.wait_recv()
    packed = 0.0
    for c in range(chunks):
        packed = packed + contract(
            take[:, c * LANES : (c + 1) * LANES], inc[c], ((1,), (1,))
        )
    pack[...] = packed.reshape(pack.shape)
    returns = []
    for k in range(1, groups):
        peer = lax.rem(c_me + k, groups)
        copy = pltpu.make_async_remote_copy(
            src_ref=pack.at[peer],
            dst_ref=land.at[c_me],
            send_sem=back_sem.at[0, k],
            recv_sem=back_sem.at[1, k],
            device_id={"col": peer},
            device_id_type=MESH,
        )
        copy.start()
        returns.append(copy)
    waits += returns
    land[c_me] = pack[c_me]
    for copy in returns:
        copy.wait_recv()
    for copy in waits:
        copy.wait_send()
    for store in stores:
        store.wait()


def finish_kernel(land_ref, give_ref, state_ref, tend_ref, final_ref, sems):
    fields = state_ref.shape[0]
    store = [
        pltpu.make_async_copy(state_ref.at[f], final_ref.at[f], sems.at[f]) for f in range(fields)
    ]
    for copy in store:
        copy.start()
    groups, cap, rows = land_ref.shape
    back = contract(land_ref[...].reshape(groups * cap, rows), give_ref[...], ((0,), (0,)))
    tend_ref[...] = back[: tend_ref.shape[0]]
    for copy in store:
        copy.wait()


def on_device(profiles, courant, owner_map, cloud_flags, crm_state):
    columns = profiles.shape[0]
    fields, levels, cells = crm_state.shape[:3]
    groups = lax.axis_size("col")
    peers = lax.axis_size("grp")
    per_peer = columns // groups
    cap = round_up(per_peer + min(2, per_peer), 8)
    chunks = columns // LANES
    depth = min(DEPTH, cells)
    rounds = STEPS // depth
    rows = round_up(fields * levels, 8 * peers)
    f32 = lambda *shape: pltpu.VMEM(shape, jnp.float32)
    dma = lambda *shape: pltpu.SemaphoreType.DMA(shape)
    vmem = pl.BlockSpec(memory_space=pltpu.VMEM)
    anywhere = pl.BlockSpec(memory_space=pl.ANY)
    tall = round_up(TOP + cells + 2 * depth + 1, 8)
    land, give, state = pl.pallas_call(
        functools.partial(window_kernel, depth),
        out_shape=(
            jax.ShapeDtypeStruct((groups, cap, rows), jnp.float32),
            jax.ShapeDtypeStruct((groups * cap, columns), jnp.float32),
            jax.ShapeDtypeStruct(crm_state.shape, jnp.float32),
        ),
        in_specs=[vmem, vmem, vmem, vmem, pl.BlockSpec(memory_space=pltpu.HBM)],
        out_specs=(vmem, vmem, anywhere),
        scratch_shapes=[
            f32(chunks, fields, levels, cells, LANES),
            f32(chunks, fields, levels, cells, LANES),
            f32(chunks, 2, fields, levels, tall, LANES),
            f32(chunks, rounds, 2, fields, levels, depth, LANES),
            f32(chunks, rounds, 2, fields, levels, depth, LANES),
            f32(groups * cap, columns),
            f32(groups, cap, 2 * LANES),
            f32(groups, cap, 2 * LANES),
            f32(chunks, fields, levels, LANES),
            f32(chunks, levels, LANES),
            f32(chunks, rows, LANES),
            f32(chunks, peers, rows // peers, LANES),
            f32(chunks, rows // peers, LANES),
            f32(chunks, rows, LANES),
            f32(groups, cap, rows),
            dma(2, chunks),
            dma(2, chunks, rounds, 2),
            dma(2, groups),
            dma(2, 2, chunks, peers),
            dma(2, groups),
        ],
        compiler_params=pltpu.CompilerParams(
            collective_id=0, has_side_effects=True, vmem_limit_bytes=LIMIT
        ),
    )(
        profiles.T,
        courant.T,
        owner_map.reshape(groups * chunks, LANES),
        cloud_flags[None, :],
        crm_state,
    )
    tendency, final = pl.pallas_call(
        finish_kernel,
        out_shape=(
            jax.ShapeDtypeStruct((fields * levels, columns), jnp.float32),
            jax.ShapeDtypeStruct(crm_state.shape, jnp.float32),
        ),
        in_specs=[vmem, vmem, anywhere],
        out_specs=(vmem, anywhere),
        scratch_shapes=[dma(fields)],
        compiler_params=pltpu.CompilerParams(vmem_limit_bytes=4 * 2**20),
    )(land, give, state)
    return tendency.T, final


def solution(mesh):
    placed = (P("col", None), P("col", None), P(), P("col"), P(None, None, "grp", "col"))
    return jax.shard_map(
        on_device,
        mesh=mesh,
        in_specs=placed,
        out_specs=(P("col", None), P(None, None, "grp", "col")),
        check_vma=False,
    )
```
